32 devices in a mesh: row: 8 (over z, y), col: 4 (over x, core).
Axes of the slice: x: 2, y: 2, z: 4, core: 2. Of those that a mesh axis runs over, the one named last changes fastest.
Arguments:
- points: float32 [16, 4096], P(None, ('col', 'row')), may hold values from -5 to 5
- inv_scales: float32 [16], replicated, may hold values from 0.1 to 0.4
- amplitude: float32 [1], replicated, may hold values from 0.5 to 2
- noise_var: float32 [1], replicated, may hold values from 0.3 to 1
- targets: float32 [8, 4096], P(None, ('col', 'row')), may hold values from -6 to 6
- initial: float32 [8, 4096], P(None, ('col', 'row')), may hold values from -3 to 3
- ritz_basis: float32 [64, 4096], P(None, ('col', 'row')), may hold values from -0.09375 to 0.09375
Outputs:
- solution: float32 [8, 4096], P(None, ('col', 'row'))
- residual: float32 [8, 4096], P(None, ('col', 'row'))
The draws below stay inside these ranges and needn't reach their ends.
All inputs are finite; a program needn't handle non-finite values.
Results may differ from the reference program's by a relative error of at most 0.00065.
Values sent between devices are 32-bit elements; how exact they have to be, the bound alone decides.
A program may use at most 128 MiB of HBM per device.

```python
import math
import jax
import jax.numpy as jnp
from jax import lax

FEAT = 16
RITZ = 64
ITERS = 1
RHS = 8
POINTS = 4096


def level_of(key, dims, cuts, low, largest):
    level = 1.0
    for axis_at, parts in cuts:
        draws = jax.random.uniform(jax.random.fold_in(jax.random.fold_in(key, 6), axis_at), (parts,), jnp.float32, low / len(cuts), largest / len(cuts))
        level = level * jnp.repeat(jnp.exp(draws), dims[axis_at] // parts).reshape((-1,) + (1,) * (len(dims) - 1 - axis_at))
    return level


def normal_values(key, extent, deviation, reach, split=(), kind=jnp.bfloat16):
    level = level_of(key, extent, split, -0.22, 0.18) if split else 1.0
    drawn = jax.random.normal(key, extent, jnp.float32) * deviation * level
    return jnp.minimum(jnp.maximum(drawn, -reach), reach).astype(kind)


def setup_inputs(seed: int = 0) -> dict:
    key_list = jax.random.split(jax.random.key(seed), 8)
    points = normal_values(key_list[0], (FEAT, POINTS), 1.0, 5.0, ((1, 32),), jnp.float32)
    inv_scales = jnp.clip(jnp.exp(jax.random.uniform(key_list[1], (FEAT,), jnp.float32, math.log(0.1), math.log(0.4))), 0.1, 0.4)
    amplitude = jnp.clip(jnp.exp(jax.random.uniform(key_list[2], (1,), jnp.float32, math.log(0.5), math.log(2.0))), 0.5, 2.0)
    noise_var = jnp.clip(jnp.exp(jax.random.uniform(key_list[3], (1,), jnp.float32, math.log(0.3), math.log(1.0))), 0.3, 1.0)
    targets = normal_values(key_list[4], (RHS, POINTS), 1.0, 6.0, ((1, 32),), jnp.float32)
    initial = normal_values(key_list[5], (RHS, POINTS), 0.5, 3.0, ((1, 32),), jnp.float32)
    ritz_basis = normal_values(key_list[6], (RITZ, POINTS), POINTS ** -0.5, 0.09375, ((1, 32),), jnp.float32)
    return dict(points=points, inv_scales=inv_scales, amplitude=amplitude, noise_var=noise_var, targets=targets, initial=initial, ritz_basis=ritz_basis)


HIGH = lax.Precision.HIGHEST

def kernel_tile(col_x, col_sq, row_x, row_sq, gain):
    cross_term = jnp.dot(col_x.T.astype(jnp.float32), row_x.astype(jnp.float32), precision=HIGH, preferred_element_type=jnp.float32)
    distance = jnp.maximum(col_sq[:, None] + row_sq[None, :] - 2.0 * cross_term, 0.0)
    return gain * jnp.exp(-0.5 * distance)

def coarse_solve(factor, rhs_block):
    middle = lax.linalg.triangular_solve(factor, rhs_block, left_side=True, lower=True)
    return lax.linalg.triangular_solve(factor, middle, left_side=True, lower=True, transpose_a=True)

def matmul(left, right):
    return jnp.dot(left.astype(jnp.float32), right.astype(jnp.float32), precision=HIGH, preferred_element_type=jnp.float32)

def apply_operator(vectors, scaled, sq_norms, gain, nugget):
    length = scaled.shape[1]
    block_size = math.gcd(length, 2048)
    num_blocks = length // block_size

    def one_block(block_index):
        offset = (block_index * block_size).astype(jnp.int32)
        row_x = lax.dynamic_slice_in_dim(scaled, offset, block_size, 1)
        row_sq = lax.dynamic_slice_in_dim(sq_norms, offset, block_size, 0)
        kernel_block = kernel_tile(scaled, sq_norms, row_x, row_sq, gain)
        return jnp.dot(vectors.astype(jnp.float32), kernel_block.astype(jnp.float32), precision=HIGH, preferred_element_type=jnp.float32)
    results = lax.map(one_block, jnp.arange(num_blocks, dtype=jnp.int32))
    results = jnp.transpose(results, (1, 0, 2)).reshape(vectors.shape[0], length)
    return results + nugget * vectors

def reference(points, inv_scales, amplitude, noise_var, targets, initial, ritz_basis):
    gain = amplitude[0]
    nugget = noise_var[0]
    scaled = points * inv_scales[:, None]
    sq_norms = jnp.sum(scaled * scaled, axis=0)
    rhs_count = initial.shape[0]
    applied_all = apply_operator(jnp.concatenate([initial, ritz_basis], 0), scaled, sq_norms, gain, nugget)
    ritz_image = applied_all[rhs_count:]
    first_residual = targets - applied_all[:rhs_count]
    coarse = matmul(ritz_basis, ritz_image.T)
    coarse = 0.5 * (coarse + coarse.T)
    projected = matmul(ritz_basis, first_residual.T)
    factor = jnp.linalg.cholesky(coarse)
    coarse_inverse = coarse_solve(factor, jnp.eye(coarse.shape[0], dtype=coarse.dtype))
    amounts = matmul(coarse_inverse, projected)
    solution = initial + matmul(amounts.T, ritz_basis)
    residual = first_residual - matmul(amounts.T, ritz_image)
    against = matmul(ritz_image, residual.T)
    sq_norm = jnp.sum(residual * residual, axis=1)
    direction = residual - matmul(matmul(coarse_inverse, against).T, ritz_basis)
    for step in range(ITERS):
        applied = apply_operator(direction, scaled, sq_norms, gain, nugget)
        step_size = sq_norm / jnp.sum(direction * applied, axis=1)
        solution = solution + step_size[:, None] * direction
        residual = residual - step_size[:, None] * applied
        against = matmul(ritz_image, residual.T)
        new_norm = jnp.sum(residual * residual, axis=1)
        correction = matmul(matmul(coarse_inverse, against).T, ritz_basis)
        direction = residual + (new_norm / sq_norm)[:, None] * direction - correction
        sq_norm = new_norm
    return (solution, residual)
```

```python
import functools

import jax
import jax.numpy as jnp
from jax import lax
from jax.experimental import pallas as pl
from jax.experimental.pallas import tpu as pltpu
from jax.sharding import PartitionSpec as P

HIGH = lax.Precision.HIGHEST
MESH = pl.DeviceIdType.MESH
VMEM = pltpu.VMEM
SMEM = pltpu.SMEM
F32 = jnp.float32
BF16 = jnp.bfloat16


def dot(left, right, dims=((1,), (0,))):
    return lax.dot_general(left, right, (dims, ((), ())), precision=HIGH, preferred_element_type=F32)


def thirds(value):
    first = value.astype(BF16)
    rest = value - first.astype(F32)
    second = rest.astype(BF16)
    third = (rest - second.astype(F32)).astype(BF16)
    return first, second, third


def augmented(scaled, swap):
    feat, width = scaled.shape
    half = -0.5 * jnp.sum(scaled * scaled, axis=0, keepdims=True)
    at = lax.broadcasted_iota(jnp.int32, (16, width), 0)
    first, second = (1, 0) if swap else (0, 1)
    tail = jnp.where(at == first, half, jnp.where(at == second, 1.0, 0.0))
    return jnp.concatenate([scaled, tail], axis=0)


def kernel(
    rows, cols, pts, scl, amp, nug, tgt, x0, w, sol_out, res_out,
    xj, xi, vj, wi, kt, ts, rs1, pscr, r1, pfull, sscr, rj, ri, agscr, ag, ts2, dscr, rs2, cscr, cv,
    send, recv,
):
    r = lax.axis_index("row")
    c = lax.axis_index("col")
    block = pts.shape[1]
    ritz = w.shape[0]
    rhs = x0.shape[0]
    count = rows * cols
    me = r * cols + c

    def lanes(at):
        return pl.ds(pl.multiple_of(at * block, block), block)

    def row_peer(k):
        return lax.rem(r + k, rows), c

    def col_peer(k):
        return r, lax.rem(c + k, cols)

    def any_peer(k):
        return lax.rem(r + k // cols, rows), lax.rem(c + k % cols, cols)

    def each(n, body):
        if n <= 32:
            for k in range(1, n):
                body(k)
        else:
            lax.fori_loop(1, n, lambda k, carry: (body(k), carry)[1], 0)

    def start(phase, src, dst, peer):
        pltpu.make_async_remote_copy(
            src_ref=src, dst_ref=dst, send_sem=send.at[phase], recv_sem=recv.at[phase],
            device_id=peer, device_id_type=MESH,
        ).start()

    def drain(phase, ref):
        return pltpu.make_async_remote_copy(
            src_ref=ref, dst_ref=ref, send_sem=send.at[phase], recv_sem=recv.at[phase],
            device_id=(r, c), device_id_type=MESH,
        )

    barrier = pltpu.get_barrier_semaphore()

    def greet(k):
        pl.semaphore_signal(barrier, inc=1, device_id=any_peer(k), device_id_type=MESH)

    each(count, greet)
    xj[:, lanes(r)] = pts[...]
    xi[:, lanes(c)] = pts[...]
    vj[pl.ds(0, ritz), lanes(r)] = w[...]
    vj[pl.ds(ritz, rhs), lanes(r)] = x0[...]
    wi[:, lanes(c)] = w[...]
    pscr[...] = jnp.zeros_like(pscr)
    agscr[...] = jnp.zeros_like(agscr)
    pl.semaphore_wait(barrier, count - 1)

    each(rows, lambda k: start(0, pts, xj.at[:, lanes(r)], row_peer(k)))
    each(cols, lambda k: start(1, pts, xi.at[:, lanes(c)], col_peer(k)))
    each(rows, lambda k: start(2, w, vj.at[pl.ds(0, ritz), lanes(r)], row_peer(k)))
    each(cols, lambda k: start(3, w, wi.at[:, lanes(c)], col_peer(k)))
    each(rows, lambda k: start(4, x0, vj.at[pl.ds(ritz, rhs), lanes(r)], row_peer(k)))

    gain = amp[0]
    nugget = nug[0]
    feat = pts.shape[0]
    at = lax.broadcasted_iota(jnp.int32, (feat, 1), 0)
    scale = jnp.zeros((feat, 1), F32)
    for k in range(feat):
        scale = jnp.where(at == k, scl[k], scale)

    others_j = pl.ds(0, (rows - 1) * block)
    others_i = pl.ds(0, (cols - 1) * block)
    drain_xi = drain(1, xi.at[:, others_i])
    drain_xj = drain(0, xj.at[:, others_j])
    drain_xi.wait_recv()
    a, b, d = thirds(augmented(xi[...] * scale, True))
    right = jnp.concatenate([a, b, d, a, b, a], axis=0)
    drain_xj.wait_recv()
    a, b, d = thirds(augmented(xj[...] * scale, False))
    left = jnp.concatenate([a, a, a, b, b, d], axis=0)
    step = 2 * block
    for base in range(0, rows * block, step):
        half_distance = lax.dot_general(
            left[:, base:base + step], right, (((0,), (0,)), ((), ())), preferred_element_type=F32
        )
        kt[base:base + step, :] = gain * jnp.exp(jnp.minimum(half_distance, 0.0))

    drain_w = drain(2, vj.at[pl.ds(0, ritz), others_j])
    drain_x0 = drain(4, vj.at[pl.ds(ritz, rhs), others_j])
    drain_wi = drain(3, wi.at[:, others_i])
    drain_w.wait_recv()
    drain_x0.wait_recv()
    ts[...] = dot(vj[...], kt[...])
    ts[pl.ds(0, ritz), lanes(c)] += nugget * w[...]
    ts[pl.ds(ritz, rhs), lanes(c)] += nugget * x0[...] - tgt[...]
    each(cols, lambda k: start(5, ts.at[:, lanes(lax.rem(c + k, cols))], rs1.at[c], col_peer(k)))
    drain_wi.wait_recv()
    gram = dot(wi[...], ts[...], ((1,), (1,)))
    part = ritz // rows
    gram = jnp.concatenate([gram, jnp.zeros((ritz, block - ritz - rhs), F32)], axis=1)
    pscr[...] = gram.reshape(rows, part, block)

    def send_part(k):
        peer = any_peer(k)
        start(6, pscr.at[peer[0]], r1.at[me], peer)

    each(count, send_part)
    r1[me] = pscr[r]
    rs1[c] = ts[:, lanes(c)]
    drain_r1 = drain(6, r1.at[pl.ds(0, count - 1)])
    drain_r1.wait_recv()
    mine = jnp.sum(r1[...], axis=0)
    sscr[...] = mine
    each(rows, lambda k: start(7, sscr, pfull.at[r], row_peer(k)))
    pfull[r] = mine
    drain_rs1 = drain(5, rs1.at[pl.ds(0, cols - 1)])
    drain_rs1.wait_recv()
    own = jnp.sum(rs1[...], axis=0)
    image = own[:ritz]
    drain_pf = drain(7, pfull.at[pl.ds(0, rows - 1)])
    drain_pf.wait_recv()
    full = pfull[...].reshape(ritz, block)

    lane = lax.broadcasted_iota(jnp.int32, (8, block), 1)
    lane_row = lax.broadcasted_iota(jnp.int32, (1, block), 1)
    sub = lax.broadcasted_iota(jnp.int32, (8, block), 0)
    pad = jnp.zeros((block - ritz, block), F32)
    flipped = jnp.concatenate([full, pad], axis=0).T[:ritz]
    tiles = []
    for i in range(ritz // 8):
        top = full[8 * i:8 * i + 8]
        tiles.append(jnp.where(lane < ritz, 0.5 * (top + flipped[8 * i:8 * i + 8]), top))
    for k in range(ritz):
        hold, inner = divmod(k, 8)
        pivot_row = tiles[hold][inner:inner + 1]
        inverse = 1.0 / pivot_row[:, k:k + 1]
        pivot_row = jnp.where(lane_row == k, 1.0, pivot_row) * inverse
        for i in range(ritz // 8):
            column = jnp.broadcast_to(tiles[i][:, k:k + 1], (8, block))
            kept = jnp.where(lane == k, 0.0, tiles[i])
            if i == hold:
                column = jnp.where(sub == inner, -1.0, column)
                kept = jnp.where(sub == inner, 0.0, kept)
            tiles[i] = kept - column * pivot_row
    turned = jnp.concatenate(tiles + [pad], axis=0).T
    inverse = turned[:ritz, :ritz]
    amounts = -turned[ritz:ritz + rhs, :ritz]
    moved = dot(amounts, jnp.concatenate([image, w[...]], axis=1))
    residual = -own[ritz:] - moved[:, :block]
    iterate = x0[...] + moved[:, block:]
    agscr[...] = jnp.concatenate(
        [dot(residual, image, ((1,), (1,))), jnp.zeros((rhs, block - ritz), F32)], axis=1
    )
    res_out[...] = residual
    rj[:, lanes(r)] = residual
    ri[:, lanes(c)] = residual
    each(count, lambda k: start(10, agscr, ag.at[me], any_peer(k)))
    each(rows, lambda k: start(8, res_out, rj.at[:, lanes(r)], row_peer(k)))
    each(cols, lambda k: start(9, res_out, ri.at[:, lanes(c)], col_peer(k)))
    ag[me] = agscr[...]
    drain_ag = drain(10, ag.at[pl.ds(0, count - 1)])
    drain_rj = drain(8, rj.at[:, others_j])
    drain_ri = drain(9, ri.at[:, others_i])
    drain_ag.wait_recv()
    against = jnp.sum(ag[...], axis=0)[:, :ritz]
    weights = dot(against, inverse)
    drain_rj.wait_recv()
    direction_j = rj[...] - dot(weights, vj[pl.ds(0, ritz), :])
    drain_ri.wait_recv()
    direction_i = ri[...] - dot(weights, wi[...])
    dscr[...] = direction_i
    direction = dscr[:, lanes(c)]
    applied_i = dot(direction_j, kt[...])
    ts2[...] = applied_i
    ts2[:, lanes(c)] += nugget * direction
    each(cols, lambda k: start(11, ts2.at[:, lanes(lax.rem(c + k, cols))], rs2.at[c], col_peer(k)))
    curve = jnp.sum(ts2[...] * direction_i, axis=1, keepdims=True)
    squares = jnp.sum(residual * residual, axis=1, keepdims=True)
    lane = lax.broadcasted_iota(jnp.int32, (rhs, block), 1)
    sub = lax.broadcasted_iota(jnp.int32, (rhs, block), 0)
    cscr[...] = jnp.sum(
        jnp.where(lane == sub, curve, jnp.where(lane == sub + rhs, squares, 0.0)), axis=0, keepdims=True
    )
    each(count, lambda k: start(12, cscr, cv.at[me], any_peer(k)))
    cv[me] = cscr[...]
    rs2[c] = ts2[:, lanes(c)]
    drain_rs2 = drain(11, rs2.at[pl.ds(0, cols - 1)])
    drain_cv = drain(12, cv.at[pl.ds(0, count - 1)])
    drain_rs2.wait_recv()
    applied = jnp.sum(rs2[...], axis=0)
    drain_cv.wait_recv()
    totals = jnp.broadcast_to(jnp.sum(cv[...], axis=0), (rhs, block))
    curve = jnp.sum(jnp.where(lane == sub, totals, 0.0), axis=1, keepdims=True)
    squares = jnp.sum(jnp.where(lane == sub + rhs, totals, 0.0), axis=1, keepdims=True)
    step_size = squares / curve
    sol_out[...] = iterate + step_size * direction
    drain_rj.wait_send()
    drain_ri.wait_send()
    res_out[...] = residual - step_size * applied
    for item in (drain_xj, drain_xi, drain_w, drain_wi, drain_x0, drain_rs1, drain_r1, drain_pf,
                 drain_ag, drain_rs2, drain_cv):
        item.wait_send()


def local(rows, cols, points, inv_scales, amplitude, noise_var, targets, initial, ritz_basis):
    feat, block = points.shape
    rhs = initial.shape[0]
    ritz = ritz_basis.shape[0]
    count = rows * cols
    vectors = rhs + ritz
    part = ritz // rows
    scratch = [
        VMEM((feat, rows * block), F32),
        VMEM((feat, cols * block), F32),
        VMEM((vectors, rows * block), F32),
        VMEM((ritz, cols * block), F32),
        VMEM((rows * block, cols * block), F32),
        VMEM((vectors, cols * block), F32),
        VMEM((cols, vectors, block), F32),
        VMEM((rows, part, block), F32),
        VMEM((count, part, block), F32),
        VMEM((rows, part, block), F32),
        VMEM((part, block), F32),
        VMEM((rhs, rows * block), F32),
        VMEM((rhs, cols * block), F32),
        VMEM((rhs, block), F32),
        VMEM((count, rhs, block), F32),
        VMEM((rhs, cols * block), F32),
        VMEM((rhs, cols * block), F32),
        VMEM((cols, rhs, block), F32),
        VMEM((1, block), F32),
        VMEM((count, 1, block), F32),
        pltpu.SemaphoreType.DMA((13,)),
        pltpu.SemaphoreType.DMA((13,)),
    ]
    vmem = pl.BlockSpec(memory_space=VMEM)
    smem = pl.BlockSpec(memory_space=SMEM)
    return pl.pallas_call(
        functools.partial(kernel, rows, cols),
        out_shape=[jax.ShapeDtypeStruct((rhs, block), F32)] * 2,
        in_specs=[vmem, smem, smem, smem, vmem, vmem, vmem],
        out_specs=[vmem, vmem],
        scratch_shapes=scratch,
        compiler_params=pltpu.CompilerParams(
            collective_id=0, has_side_effects=True, vmem_limit_bytes=48 * 1024 * 1024
        ),
        name="deflated_cg",
    )(points, inv_scales, amplitude, noise_var, targets, initial, ritz_basis)


def solution(mesh):
    spread = P(None, ("col", "row"))
    return jax.shard_map(
        functools.partial(local, mesh.shape["row"], mesh.shape["col"]),
        mesh=mesh,
        in_specs=(spread, P(), P(), P(), spread, spread, spread),
        out_specs=(spread, spread),
        check_vma=False,
    )
```

```python
import functools

import jax
import jax.numpy as jnp
from jax import lax
from jax.experimental import pallas as pl
from jax.experimental.pallas import tpu as pltpu
from jax.sharding import PartitionSpec as P

HIGH = lax.Precision.HIGHEST
MESH = pl.DeviceIdType.MESH
VMEM = pltpu.VMEM
SMEM = pltpu.SMEM
F32 = jnp.float32
BF16 = jnp.bfloat16


def dot(left, right, dims=((1,), (0,))):
    return lax.dot_general(left, right, (dims, ((), ())), precision=HIGH, preferred_element_type=F32)


def thirds(value):
    first = value.astype(BF16)
    rest = value - first.astype(F32)
    second = rest.astype(BF16)
    third = (rest - second.astype(F32)).astype(BF16)
    return first, second, third


def augmented(scaled, swap):
    feat, width = scaled.shape
    half = -0.5 * jnp.sum(scaled * scaled, axis=0, keepdims=True)
    at = lax.broadcasted_iota(jnp.int32, (16, width), 0)
    first, second = (1, 0) if swap else (0, 1)
    tail = jnp.where(at == first, half, jnp.where(at == second, 1.0, 0.0))
    return jnp.concatenate([scaled, tail], axis=0)


def kernel(
    high, low, cols, pts_in, scl_in, amp_in, nug_in, tgt_in, x0_in, w_in, out,
    pts, scl, amp, nug, tgt, x0, w, res,
    xj, xi, vj, wi, kt, ts, rs1, pscr, r1, pfull, sscr, rj, ri, agscr, ag, ts2, dscr, rs2, cscr, cv,
    loads, send, recv,
):
    rows = low * cols
    me = lax.axis_index("row") * cols + lax.axis_index("col")
    h = me // rows
    j = lax.rem(me, rows)
    block = pts.shape[1]
    ritz = w.shape[0]
    rhs = x0.shape[0]
    count = high * rows

    fetches = [
        pltpu.make_async_copy(src, dst, loads.at[k])
        for k, (src, dst) in enumerate(
            ((pts_in, pts), (w_in, w), (x0_in, x0), (tgt_in, tgt), (scl_in, scl), (amp_in, amp), (nug_in, nug))
        )
    ]
    for fetch in fetches:
        fetch.start()

    def lanes(at):
        return pl.ds(pl.multiple_of(at * block, block), block)

    def place(flat):
        return flat // cols, lax.rem(flat, cols)

    def row_peer(k):
        return place(h * rows + lax.rem(j + k, rows))

    def col_peer(k):
        return place(lax.rem(h + k, high) * rows + j)

    def any_peer(k):
        return place(lax.rem(me + k, count))

    def each(n, body):
        if n <= 32:
            for k in range(1, n):
                body(k)
        else:
            lax.fori_loop(1, n, lambda k, carry: (body(k), carry)[1], 0)

    def start(phase, src, dst, peer):
        pltpu.make_async_remote_copy(
            src_ref=src, dst_ref=dst, send_sem=send.at[phase], recv_sem=recv.at[phase],
            device_id=peer, device_id_type=MESH,
        ).start()

    def drain(phase, ref):
        return pltpu.make_async_remote_copy(
            src_ref=ref, dst_ref=ref, send_sem=send.at[phase], recv_sem=recv.at[phase],
            device_id=place(me), device_id_type=MESH,
        )

    barrier = pltpu.get_barrier_semaphore()

    def greet(peer):
        pl.semaphore_signal(barrier, inc=1, device_id=peer, device_id_type=MESH)

    each(high, lambda k: greet(col_peer(k)))
    each(rows, lambda k: greet(row_peer(k)))
    pscr[...] = jnp.zeros_like(pscr)
    agscr[...] = jnp.zeros_like(agscr)
    for fetch in fetches:
        fetch.wait()
    xj[:, lanes(j)] = pts[...]
    xi[:, lanes(h)] = pts[...]
    vj[pl.ds(0, ritz), lanes(j)] = w[...]
    vj[pl.ds(ritz, rhs), lanes(j)] = x0[...]
    wi[:, lanes(h)] = w[...]
    pl.semaphore_wait(barrier, high + rows - 2)

    each(rows, lambda k: start(0, pts, xj.at[:, lanes(j)], row_peer(k)))
    each(high, lambda k: start(1, pts, xi.at[:, lanes(h)], col_peer(k)))
    each(rows, lambda k: start(2, w, vj.at[pl.ds(0, ritz), lanes(j)], row_peer(k)))
    each(high, lambda k: start(3, w, wi.at[:, lanes(h)], col_peer(k)))
    each(rows, lambda k: start(4, x0, vj.at[pl.ds(ritz, rhs), lanes(j)], row_peer(k)))

    gain = amp[0]
    nugget = nug[0]
    feat = pts.shape[0]
    at = lax.broadcasted_iota(jnp.int32, (feat, 1), 0)
    scale = jnp.zeros((feat, 1), F32)
    for k in range(feat):
        scale = jnp.where(at == k, scl[k], scale)

    others_j = pl.ds(0, (rows - 1) * block)
    others_i = pl.ds(0, (high - 1) * block)
    drain_xi = drain(1, xi.at[:, others_i])
    drain_xj = drain(0, xj.at[:, others_j])
    drain_xi.wait_recv()
    a, b, d = thirds(augmented(xi[...] * scale, True))
    right = jnp.concatenate([a, b, d, a, b, a], axis=0)
    drain_xj.wait_recv()
    a, b, d = thirds(augmented(xj[...] * scale, False))
    left = jnp.concatenate([a, a, a, b, b, d], axis=0)
    step = 2 * block
    for base in range(0, rows * block, step):
        half_distance = lax.dot_general(
            left[:, base:base + step], right, (((0,), (0,)), ((), ())), preferred_element_type=F32
        )
        kt[base:base + step, :] = gain * jnp.exp(jnp.minimum(half_distance, 0.0))

    drain_w = drain(2, vj.at[pl.ds(0, ritz), others_j])
    drain_x0 = drain(4, vj.at[pl.ds(ritz, rhs), others_j])
    drain_wi = drain(3, wi.at[:, others_i])
    drain_w.wait_recv()
    drain_x0.wait_recv()
    ts[...] = dot(vj[...], kt[...])
    ts[pl.ds(0, ritz), lanes(h)] += nugget * w[...]
    ts[pl.ds(ritz, rhs), lanes(h)] += nugget * x0[...] - tgt[...]
    each(high, lambda k: start(5, ts.at[:, lanes(lax.rem(h + k, high))], rs1.at[h], col_peer(k)))
    drain_wi.wait_recv()
    gram = dot(wi[...], ts[...], ((1,), (1,)))
    part = ritz // rows
    gram = jnp.concatenate([gram, jnp.zeros((ritz, block - ritz - rhs), F32)], axis=1)
    pscr[...] = gram.reshape(rows, part, block)

    def send_part(k):
        start(6, pscr.at[lax.rem(j + k, rows)], r1.at[me], any_peer(k))

    each(count, send_part)
    r1[me] = pscr[j]
    rs1[h] = ts[:, lanes(h)]
    drain_r1 = drain(6, r1.at[pl.ds(0, count - 1)])
    drain_r1.wait_recv()
    mine = jnp.sum(r1[...], axis=0)
    sscr[...] = mine
    each(rows, lambda k: start(7, sscr, pfull.at[j], row_peer(k)))
    pfull[j] = mine
    drain_rs1 = drain(5, rs1.at[pl.ds(0, high - 1)])
    drain_rs1.wait_recv()
    own = jnp.sum(rs1[...], axis=0)
    image = own[:ritz]
    drain_pf = drain(7, pfull.at[pl.ds(0, rows - 1)])
    drain_pf.wait_recv()
    full = pfull[...].reshape(ritz, block)

    lane = lax.broadcasted_iota(jnp.int32, (8, block), 1)
    lane_row = lax.broadcasted_iota(jnp.int32, (1, block), 1)
    sub = lax.broadcasted_iota(jnp.int32, (8, block), 0)
    pad = jnp.zeros((block - ritz, block), F32)
    flipped = jnp.concatenate([full, pad], axis=0).T[:ritz]
    tiles = []
    for i in range(ritz // 8):
        top = full[8 * i:8 * i + 8]
        tiles.append(jnp.where(lane < ritz, 0.5 * (top + flipped[8 * i:8 * i + 8]), top))
    for k in range(ritz):
        hold, inner = divmod(k, 8)
        pivot_row = tiles[hold][inner:inner + 1]
        inverse = 1.0 / pivot_row[:, k:k + 1]
        pivot_row = jnp.where(lane_row == k, 1.0, pivot_row) * inverse
        for i in range(ritz // 8):
            column = jnp.broadcast_to(tiles[i][:, k:k + 1], (8, block))
            kept = jnp.where(lane == k, 0.0, tiles[i])
            if i == hold:
                column = jnp.where(sub == inner, -1.0, column)
                kept = jnp.where(sub == inner, 0.0, kept)
            tiles[i] = kept - column * pivot_row
    turned = jnp.concatenate(tiles + [pad], axis=0).T
    inverse = turned[:ritz, :ritz]
    amounts = -turned[ritz:ritz + rhs, :ritz]
    moved = dot(amounts, jnp.concatenate([image, w[...]], axis=1))
    residual = -own[ritz:] - moved[:, :block]
    iterate = x0[...] + moved[:, block:]
    agscr[...] = jnp.concatenate(
        [dot(residual, image, ((1,), (1,))), jnp.zeros((rhs, block - ritz), F32)], axis=1
    )
    res[...] = residual
    rj[:, lanes(j)] = residual
    ri[:, lanes(h)] = residual
    each(count, lambda k: start(10, agscr, ag.at[me], any_peer(k)))
    each(rows, lambda k: start(8, res, rj.at[:, lanes(j)], row_peer(k)))
    each(high, lambda k: start(9, res, ri.at[:, lanes(h)], col_peer(k)))
    ag[me] = agscr[...]
    drain_ag = drain(10, ag.at[pl.ds(0, count - 1)])
    drain_rj = drain(8, rj.at[:, others_j])
    drain_ri = drain(9, ri.at[:, others_i])
    drain_ag.wait_recv()
    against = jnp.sum(ag[...], axis=0)[:, :ritz]
    weights = dot(against, inverse)
    drain_rj.wait_recv()
    direction_j = rj[...] - dot(weights, vj[pl.ds(0, ritz), :])
    drain_ri.wait_recv()
    direction_i = ri[...] - dot(weights, wi[...])
    dscr[...] = direction_i
    direction = dscr[:, lanes(h)]
    applied_i = dot(direction_j, kt[...])
    ts2[...] = applied_i
    ts2[:, lanes(h)] += nugget * direction
    each(high, lambda k: start(11, ts2.at[:, lanes(lax.rem(h + k, high))], rs2.at[h], col_peer(k)))
    curve = jnp.sum(ts2[...] * direction_i, axis=1, keepdims=True)
    squares = jnp.sum(residual * residual, axis=1, keepdims=True)
    lane = lax.broadcasted_iota(jnp.int32, (rhs, block), 1)
    sub = lax.broadcasted_iota(jnp.int32, (rhs, block), 0)
    cscr[...] = jnp.sum(
        jnp.where(lane == sub, curve, jnp.where(lane == sub + rhs, squares, 0.0)), axis=0, keepdims=True
    )
    each(count, lambda k: start(12, cscr, cv.at[me], any_peer(k)))
    cv[me] = cscr[...]
    rs2[h] = ts2[:, lanes(h)]
    drain_rs2 = drain(11, rs2.at[pl.ds(0, high - 1)])
    drain_cv = drain(12, cv.at[pl.ds(0, count - 1)])
    drain_rs2.wait_recv()
    applied = jnp.sum(rs2[...], axis=0)
    drain_cv.wait_recv()
    totals = jnp.broadcast_to(jnp.sum(cv[...], axis=0), (rhs, block))
    curve = jnp.sum(jnp.where(lane == sub, totals, 0.0), axis=1, keepdims=True)
    squares = jnp.sum(jnp.where(lane == sub + rhs, totals, 0.0), axis=1, keepdims=True)
    step_size = squares / curve
    out[pl.ds(0, rhs)] = iterate + step_size * direction
    out[pl.ds(rhs, rhs)] = residual - step_size * applied
    for item in (drain_rj, drain_ri, drain_xj, drain_xi, drain_w, drain_wi, drain_x0, drain_rs1, drain_r1, drain_pf,
                 drain_ag, drain_rs2, drain_cv):
        item.wait_send()


def local(high, low, cols, points, inv_scales, amplitude, noise_var, targets, initial, ritz_basis):
    feat, block = points.shape
    rhs = initial.shape[0]
    ritz = ritz_basis.shape[0]
    rows = low * cols
    count = high * rows
    vectors = rhs + ritz
    part = ritz // rows
    scratch = [
        VMEM((feat, block), F32),
        SMEM((feat,), F32),
        SMEM((1,), F32),
        SMEM((1,), F32),
        VMEM((rhs, block), F32),
        VMEM((rhs, block), F32),
        VMEM((ritz, block), F32),
        VMEM((rhs, block), F32),
        VMEM((feat, rows * block), F32),
        VMEM((feat, high * block), F32),
        VMEM((vectors, rows * block), F32),
        VMEM((ritz, high * block), F32),
        VMEM((rows * block, high * block), F32),
        VMEM((vectors, high * block), F32),
        VMEM((high, vectors, block), F32),
        VMEM((rows, part, block), F32),
        VMEM((count, part, block), F32),
        VMEM((rows, part, block), F32),
        VMEM((part, block), F32),
        VMEM((rhs, rows * block), F32),
        VMEM((rhs, high * block), F32),
        VMEM((rhs, block), F32),
        VMEM((count, rhs, block), F32),
        VMEM((rhs, high * block), F32),
        VMEM((rhs, high * block), F32),
        VMEM((high, rhs, block), F32),
        VMEM((1, block), F32),
        VMEM((count, 1, block), F32),
        pltpu.SemaphoreType.DMA((7,)),
        pltpu.SemaphoreType.DMA((13,)),
        pltpu.SemaphoreType.DMA((13,)),
    ]
    hbm = pl.BlockSpec(memory_space=pltpu.HBM)
    out = pl.pallas_call(
        functools.partial(kernel, high, low, cols),
        out_shape=jax.ShapeDtypeStruct((2 * rhs, block), F32),
        in_specs=[hbm] * 7,
        out_specs=pl.BlockSpec(memory_space=VMEM),
        scratch_shapes=scratch,
        compiler_params=pltpu.CompilerParams(
            collective_id=0, has_side_effects=True
        ),
        name="deflated_cg",
    )(points, inv_scales, amplitude, noise_var, targets, initial, ritz_basis)
    return out[:rhs], out[rhs:]


def solution(mesh):
    spread = P(None, ("col", "row"))
    rows, cols = mesh.shape["row"], mesh.shape["col"]
    low = next(d for d in range(1, rows + 1) if rows % d == 0 and d * cols >= rows // d)
    return jax.shard_map(
        functools.partial(local, rows // low, low, cols),
        mesh=mesh,
        in_specs=(spread, P(), P(), P(), spread, spread, spread),
        out_specs=(spread, spread),
        check_vma=False,
    )
```

```python
import functools

import jax
import jax.numpy as jnp
from jax import lax
from jax.experimental import pallas as pl
from jax.experimental.pallas import tpu as pltpu
from jax.sharding import PartitionSpec as P

HIGH = lax.Precision.HIGHEST
MESH = pl.DeviceIdType.MESH
VMEM = pltpu.VMEM
SMEM = pltpu.SMEM
F32 = jnp.float32
BF16 = jnp.bfloat16


def dot(left, right, dims=((1,), (0,))):
    return lax.dot_general(left, right, (dims, ((), ())), precision=HIGH, preferred_element_type=F32)


def thirds(value):
    first = value.astype(BF16)
    rest = value - first.astype(F32)
    second = rest.astype(BF16)
    third = (rest - second.astype(F32)).astype(BF16)
    return first, second, third


def augmented(scaled, swap):
    feat, width = scaled.shape
    half = -0.5 * jnp.sum(scaled * scaled, axis=0, keepdims=True)
    at = lax.broadcasted_iota(jnp.int32, (16, width), 0)
    first, second = (1, 0) if swap else (0, 1)
    tail = jnp.where(at == first, half, jnp.where(at == second, 1.0, 0.0))
    return jnp.concatenate([scaled, tail], axis=0)


def kernel(
    high, low, cols, pts_in, scl_in, amp_in, nug_in, tgt_in, x0_in, w_in, out,
    pts, scl, amp, nug, tgt, x0, w, res,
    xj, xi, vj, wi, kt, ts, rs1, pscr, r1, pfull, sscr, rj, ri, agscr, ag, ts2, dscr, rs2, cscr, cv,
    loads, send, recv,
):
    rows = low * cols
    me = lax.axis_index("row") * cols + lax.axis_index("col")
    h = me // rows
    j = lax.rem(me, rows)
    block = pts.shape[1]
    ritz = w.shape[0]
    rhs = x0.shape[0]
    count = high * rows

    fetches = [
        pltpu.make_async_copy(src, dst, loads.at[k])
        for k, (src, dst) in enumerate(
            ((pts_in, pts), (w_in, w), (x0_in, x0), (tgt_in, tgt), (scl_in, scl), (amp_in, amp), (nug_in, nug))
        )
    ]
    for fetch in fetches:
        fetch.start()

    def lanes(at):
        return pl.ds(pl.multiple_of(at * block, block), block)

    def place(flat):
        return flat // cols, lax.rem(flat, cols)

    def row_peer(k):
        return place(h * rows + lax.rem(j + k, rows))

    def col_peer(k):
        return place(lax.rem(h + k, high) * rows + j)

    def any_peer(k):
        return place(lax.rem(me + k, count))

    def each(n, body):
        if n <= 32:
            for k in range(1, n):
                body(k)
        else:
            lax.fori_loop(1, n, lambda k, carry: (body(k), carry)[1], 0)

    def start(phase, src, dst, peer):
        pltpu.make_async_remote_copy(
            src_ref=src, dst_ref=dst, send_sem=send.at[phase], recv_sem=recv.at[phase],
            device_id=peer, device_id_type=MESH,
        ).start()

    def drain(phase, ref):
        return pltpu.make_async_remote_copy(
            src_ref=ref, dst_ref=ref, send_sem=send.at[phase], recv_sem=recv.at[phase],
            device_id=place(me), device_id_type=MESH,
        )

    barrier = pltpu.get_barrier_semaphore()

    def greet(peer):
        pl.semaphore_signal(barrier, inc=1, device_id=peer, device_id_type=MESH)

    each(high, lambda k: greet(col_peer(k)))
    each(rows, lambda k: greet(row_peer(k)))
    for fetch in fetches:
        fetch.wait()
    xj[:, lanes(j)] = pts[...]
    xi[:, lanes(h)] = pts[...]
    vj[pl.ds(0, ritz), lanes(j)] = w[...]
    vj[pl.ds(ritz, rhs), lanes(j)] = x0[...]
    wi[:, lanes(h)] = w[...]
    pl.semaphore_wait(barrier, high + rows - 2)

    each(rows, lambda k: start(0, pts, xj.at[:, lanes(j)], row_peer(k)))
    each(high, lambda k: start(1, pts, xi.at[:, lanes(h)], col_peer(k)))
    each(rows, lambda k: start(2, w, vj.at[pl.ds(0, ritz), lanes(j)], row_peer(k)))
    each(high, lambda k: start(3, w, wi.at[:, lanes(h)], col_peer(k)))
    each(rows, lambda k: start(4, x0, vj.at[pl.ds(ritz, rhs), lanes(j)], row_peer(k)))

    gain = amp[0]
    nugget = nug[0]
    feat = pts.shape[0]
    at = lax.broadcasted_iota(jnp.int32, (feat, 1), 0)
    scale = jnp.zeros((feat, 1), F32)
    for k in range(feat):
        scale = jnp.where(at == k, scl[k], scale)

    others_j = pl.ds(0, (rows - 1) * block)
    others_i = pl.ds(0, (high - 1) * block)
    drain_xi = drain(1, xi.at[:, others_i])
    drain_xj = drain(0, xj.at[:, others_j])
    drain_xi.wait_recv()
    a, b, d = thirds(augmented(xi[...] * scale, True))
    right = jnp.concatenate([a, b, d, a, b, a], axis=0)
    drain_xj.wait_recv()
    a, b, d = thirds(augmented(xj[...] * scale, False))
    left = jnp.concatenate([a, a, a, b, b, d], axis=0)
    step = 2 * block
    for base in range(0, rows * block, step):
        half_distance = lax.dot_general(
            left[:, base:base + step], right, (((0,), (0,)), ((), ())), preferred_element_type=F32
        )
        kt[base:base + step, :] = gain * jnp.exp(jnp.minimum(half_distance, 0.0))

    drain_w = drain(2, vj.at[pl.ds(0, ritz), others_j])
    drain_x0 = drain(4, vj.at[pl.ds(ritz, rhs), others_j])
    drain_wi = drain(3, wi.at[:, others_i])
    drain_w.wait_recv()
    drain_x0.wait_recv()
    ts[...] = dot(vj[...], kt[...])
    ts[pl.ds(0, ritz), lanes(h)] += nugget * w[...]
    ts[pl.ds(ritz, rhs), lanes(h)] += nugget * x0[...] - tgt[...]
    drain_wi.wait_recv()
    gram = dot(wi[...], ts[...], ((1,), (1,)))
    part = ritz // rows
    gram = jnp.concatenate([gram, jnp.zeros((ritz, block - ritz - rhs), F32)], axis=1)
    pscr[...] = gram.reshape(rows, part, block)

    def send_part(k):
        start(6, pscr.at[lax.rem(j + k, rows)], r1.at[me], any_peer(k))

    each(count, send_part)
    each(high, lambda k: start(5, ts.at[:, lanes(lax.rem(h + k, high))], rs1.at[h], col_peer(k)))
    r1[me] = pscr[j]
    rs1[h] = ts[:, lanes(h)]
    drain_r1 = drain(6, r1.at[pl.ds(0, count - 1)])
    drain_r1.wait_recv()
    mine = jnp.sum(r1[...], axis=0)
    sscr[...] = mine
    each(rows, lambda k: start(7, sscr, pfull.at[j], row_peer(k)))
    pfull[j] = mine
    drain_rs1 = drain(5, rs1.at[pl.ds(0, high - 1)])
    drain_rs1.wait_recv()
    own = jnp.sum(rs1[...], axis=0)
    image = own[:ritz]
    drain_pf = drain(7, pfull.at[pl.ds(0, rows - 1)])
    drain_pf.wait_recv()
    full = pfull[...].reshape(ritz, block)

    lane = lax.broadcasted_iota(jnp.int32, (8, block), 1)
    lane_row = lax.broadcasted_iota(jnp.int32, (1, block), 1)
    sub = lax.broadcasted_iota(jnp.int32, (8, block), 0)
    pad = jnp.zeros((block - ritz, block), F32)
    flipped = jnp.concatenate([full, pad], axis=0).T[:ritz]
    tiles = []
    for i in range(ritz // 8):
        top = full[8 * i:8 * i + 8]
        tiles.append(jnp.where(lane < ritz, 0.5 * (top + flipped[8 * i:8 * i + 8]), top))
    for k in range(0, ritz, 2):
        hold, inner = divmod(k, 8)
        upper = tiles[hold][inner:inner + 1]
        lower = tiles[hold][inner + 1:inner + 2]
        a, b = upper[:, k:k + 1], upper[:, k + 1:k + 2]
        d, e = lower[:, k:k + 1], lower[:, k + 1:k + 2]
        inverse = 1.0 / (a * e - b * d)
        first, second = lane_row == k, lane_row == k + 1
        upper = jnp.where(first, 1.0, jnp.where(second, 0.0, upper))
        lower = jnp.where(first, 0.0, jnp.where(second, 1.0, lower))
        upper, lower = (e * inverse) * upper - (b * inverse) * lower, (a * inverse) * lower - (d * inverse) * upper
        for i in range(ritz // 8):
            left = jnp.broadcast_to(tiles[i][:, k:k + 1], (8, block))
            right = jnp.broadcast_to(tiles[i][:, k + 1:k + 2], (8, block))
            kept = jnp.where((lane == k) | (lane == k + 1), 0.0, tiles[i])
            if i == hold:
                pivots = (sub == inner) | (sub == inner + 1)
                left = jnp.where(pivots, jnp.where(sub == inner, -1.0, 0.0), left)
                right = jnp.where(pivots, jnp.where(sub == inner, 0.0, -1.0), right)
                kept = jnp.where(pivots, 0.0, kept)
            tiles[i] = (kept - left * upper) - right * lower
    turned = jnp.concatenate(tiles + [pad], axis=0).T
    inverse = turned[:ritz, :ritz]
    amounts = -turned[ritz:ritz + rhs, :ritz]
    moved = dot(amounts, jnp.concatenate([image, w[...]], axis=1))
    residual = -own[ritz:] - moved[:, :block]
    iterate = x0[...] + moved[:, block:]
    against = dot(residual, image, ((1,), (1,)))
    packed = agscr.shape[0]
    agscr[...] = jnp.concatenate([against[i:i + packed] for i in range(0, rhs, packed)], axis=1)
    res[...] = residual
    rj[:, lanes(j)] = residual
    ri[:, lanes(h)] = residual
    each(count, lambda k: start(10, agscr, ag.at[me], any_peer(k)))
    each(rows, lambda k: start(8, res, rj.at[:, lanes(j)], row_peer(k)))
    each(high, lambda k: start(9, res, ri.at[:, lanes(h)], col_peer(k)))
    ag[me] = agscr[...]
    drain_ag = drain(10, ag.at[pl.ds(0, count - 1)])
    drain_rj = drain(8, rj.at[:, others_j])
    drain_ri = drain(9, ri.at[:, others_i])
    drain_ag.wait_recv()
    against = jnp.sum(ag[...], axis=0)
    against = jnp.concatenate([against[:, i:i + ritz] for i in range(0, block, ritz)], axis=0)
    weights = dot(against, inverse)
    drain_rj.wait_recv()
    direction_j = rj[...] - dot(weights, vj[pl.ds(0, ritz), :])
    drain_ri.wait_recv()
    direction_i = ri[...] - dot(weights, wi[...])
    dscr[...] = direction_i
    direction = dscr[:, lanes(h)]
    applied_i = dot(direction_j, kt[...])
    ts2[...] = applied_i
    ts2[:, lanes(h)] += nugget * direction
    each(high, lambda k: start(11, ts2.at[:, lanes(lax.rem(h + k, high))], rs2.at[h], col_peer(k)))
    curve = jnp.sum(ts2[...] * direction_i, axis=1, keepdims=True)
    squares = jnp.sum(residual * residual, axis=1, keepdims=True)
    lane = lax.broadcasted_iota(jnp.int32, (rhs, block), 1)
    sub = lax.broadcasted_iota(jnp.int32, (rhs, block), 0)
    cscr[...] = jnp.sum(
        jnp.where(lane == sub, curve, jnp.where(lane == sub + rhs, squares, 0.0)), axis=0, keepdims=True
    )
    each(count, lambda k: start(12, cscr, cv.at[me], any_peer(k)))
    cv[me] = cscr[...]
    rs2[h] = ts2[:, lanes(h)]
    drain_rs2 = drain(11, rs2.at[pl.ds(0, high - 1)])
    drain_cv = drain(12, cv.at[pl.ds(0, count - 1)])
    drain_rs2.wait_recv()
    applied = jnp.sum(rs2[...], axis=0)
    drain_cv.wait_recv()
    totals = jnp.broadcast_to(jnp.sum(cv[...], axis=0), (rhs, block))
    curve = jnp.sum(jnp.where(lane == sub, totals, 0.0), axis=1, keepdims=True)
    squares = jnp.sum(jnp.where(lane == sub + rhs, totals, 0.0), axis=1, keepdims=True)
    step_size = squares / curve
    out[pl.ds(0, rhs)] = iterate + step_size * direction
    out[pl.ds(rhs, rhs)] = residual - step_size * applied
    for item in (drain_rj, drain_ri, drain_xj, drain_xi, drain_w, drain_wi, drain_x0, drain_rs1, drain_r1, drain_pf,
                 drain_ag, drain_rs2, drain_cv):
        item.wait_send()


def local(high, low, cols, points, inv_scales, amplitude, noise_var, targets, initial, ritz_basis):
    feat, block = points.shape
    rhs = initial.shape[0]
    ritz = ritz_basis.shape[0]
    rows = low * cols
    count = high * rows
    vectors = rhs + ritz
    part = ritz // rows
    packed = rhs * ritz // block
    scratch = [
        VMEM((feat, block), F32),
        SMEM((feat,), F32),
        SMEM((1,), F32),
        SMEM((1,), F32),
        VMEM((rhs, block), F32),
        VMEM((rhs, block), F32),
        VMEM((ritz, block), F32),
        VMEM((rhs, block), F32),
        VMEM((feat, rows * block), F32),
        VMEM((feat, high * block), F32),
        VMEM((vectors, rows * block), F32),
        VMEM((ritz, high * block), F32),
        VMEM((rows * block, high * block), F32),
        VMEM((vectors, high * block), F32),
        VMEM((high, vectors, block), F32),
        VMEM((rows, part, block), F32),
        VMEM((count, part, block), F32),
        VMEM((rows, part, block), F32),
        VMEM((part, block), F32),
        VMEM((rhs, rows * block), F32),
        VMEM((rhs, high * block), F32),
        VMEM((packed, block), F32),
        VMEM((count, packed, block), F32),
        VMEM((rhs, high * block), F32),
        VMEM((rhs, high * block), F32),
        VMEM((high, rhs, block), F32),
        VMEM((1, block), F32),
        VMEM((count, 1, block), F32),
        pltpu.SemaphoreType.DMA((7,)),
        pltpu.SemaphoreType.DMA((13,)),
        pltpu.SemaphoreType.DMA((13,)),
    ]
    hbm = pl.BlockSpec(memory_space=pltpu.HBM)
    out = pl.pallas_call(
        functools.partial(kernel, high, low, cols),
        out_shape=jax.ShapeDtypeStruct((2 * rhs, block), F32),
        in_specs=[hbm] * 7,
        out_specs=pl.BlockSpec(memory_space=VMEM),
        scratch_shapes=scratch,
        compiler_params=pltpu.CompilerParams(
            collective_id=0, has_side_effects=True
        ),
        name="deflated_cg",
    )(points, inv_scales, amplitude, noise_var, targets, initial, ritz_basis)
    return out[:rhs], out[rhs:]


def solution(mesh):
    spread = P(None, ("col", "row"))
    rows, cols = mesh.shape["row"], mesh.shape["col"]
    low = next(d for d in range(1, rows + 1) if rows % d == 0 and d * cols >= rows // d)
    return jax.shard_map(
        functools.partial(local, rows // low, low, cols),
        mesh=mesh,
        in_specs=(spread, P(), P(), P(), spread, spread, spread),
        out_specs=(spread, spread),
        check_vma=False,
    )
```

```python
import functools

import jax
import jax.numpy as jnp
from jax import lax
from jax.experimental import pallas as pl
from jax.experimental.pallas import tpu as pltpu
from jax.sharding import PartitionSpec as P

HIGH = lax.Precision.HIGHEST
MESH = pl.DeviceIdType.MESH
VMEM = pltpu.VMEM
SMEM = pltpu.SMEM
F32 = jnp.float32
BF16 = jnp.bfloat16


def dot(left, right, dims=((1,), (0,))):
    return lax.dot_general(left, right, (dims, ((), ())), precision=HIGH, preferred_element_type=F32)


def thirds(value):
    first = value.astype(BF16)
    rest = value - first.astype(F32)
    second = rest.astype(BF16)
    third = (rest - second.astype(F32)).astype(BF16)
    return first, second, third


def augmented(scaled, swap):
    feat, width = scaled.shape
    half = -0.5 * jnp.sum(scaled * scaled, axis=0, keepdims=True)
    at = lax.broadcasted_iota(jnp.int32, (16, width), 0)
    first, second = (1, 0) if swap else (0, 1)
    tail = jnp.where(at == first, half, jnp.where(at == second, 1.0, 0.0))
    return jnp.concatenate([scaled, tail], axis=0)


def kernel(
    high, low, cols, pts_in, scl_in, amp_in, nug_in, tgt_in, x0_in, w_in, out,
    pts, scl, amp, nug, tgt, x0, w, res,
    xj, xi, vj, wi, kt, ts, rs1, pscr, r1, pfull, sscr, rj, ri, agscr, ag, ts2, dscr, rs2, cscr, cv,
    loads, send, recv,
):
    rows = low * cols
    me = lax.axis_index("row") * cols + lax.axis_index("col")
    h = me // rows
    j = lax.rem(me, rows)
    block = pts.shape[1]
    ritz = w.shape[0]
    rhs = x0.shape[0]
    count = high * rows

    fetches = [
        pltpu.make_async_copy(src, dst, loads.at[k])
        for k, (src, dst) in enumerate(
            ((pts_in, pts), (w_in, w), (x0_in, x0), (tgt_in, tgt), (scl_in, scl), (amp_in, amp), (nug_in, nug))
        )
    ]
    for fetch in fetches:
        fetch.start()

    def lanes(at):
        return pl.ds(pl.multiple_of(at * block, block), block)

    def place(flat):
        return flat // cols, lax.rem(flat, cols)

    def row_peer(k):
        return place(h * rows + lax.rem(j + k, rows))

    def col_peer(k):
        return place(lax.rem(h + k, high) * rows + j)

    def any_peer(k):
        return place(lax.rem(me + k, count))

    def each(n, body):
        if n <= 32:
            for k in range(1, n):
                body(k)
        else:
            lax.fori_loop(1, n, lambda k, carry: (body(k), carry)[1], 0)

    def start(phase, src, dst, peer):
        pltpu.make_async_remote_copy(
            src_ref=src, dst_ref=dst, send_sem=send.at[phase], recv_sem=recv.at[phase],
            device_id=peer, device_id_type=MESH,
        ).start()

    def drain(phase, ref):
        return pltpu.make_async_remote_copy(
            src_ref=ref, dst_ref=ref, send_sem=send.at[phase], recv_sem=recv.at[phase],
            device_id=place(me), device_id_type=MESH,
        )

    barrier = pltpu.get_barrier_semaphore()

    def greet(peer):
        pl.semaphore_signal(barrier, inc=1, device_id=peer, device_id_type=MESH)

    each(high, lambda k: greet(col_peer(k)))
    each(rows, lambda k: greet(row_peer(k)))
    for fetch in fetches:
        fetch.wait()
    xj[:, lanes(j)] = pts[...]
    xi[:, lanes(h)] = pts[...]
    vj[pl.ds(0, ritz), lanes(j)] = w[...]
    vj[pl.ds(ritz, rhs), lanes(j)] = x0[...]
    wi[:, lanes(h)] = w[...]
    pl.semaphore_wait(barrier, high + rows - 2)

    each(rows, lambda k: start(0, pts, xj.at[:, lanes(j)], row_peer(k)))
    each(high, lambda k: start(1, pts, xi.at[:, lanes(h)], col_peer(k)))
    each(rows, lambda k: start(2, w, vj.at[pl.ds(0, ritz), lanes(j)], row_peer(k)))
    each(high, lambda k: start(3, w, wi.at[:, lanes(h)], col_peer(k)))
    each(rows, lambda k: start(4, x0, vj.at[pl.ds(ritz, rhs), lanes(j)], row_peer(k)))

    gain = amp[0]
    nugget = nug[0]
    feat = pts.shape[0]
    at = lax.broadcasted_iota(jnp.int32, (feat, 1), 0)
    scale = jnp.zeros((feat, 1), F32)
    for k in range(feat):
        scale = jnp.where(at == k, scl[k], scale)

    others_j = pl.ds(0, (rows - 1) * block)
    others_i = pl.ds(0, (high - 1) * block)
    drain_xi = drain(1, xi.at[:, others_i])
    drain_xj = drain(0, xj.at[:, others_j])
    drain_xi.wait_recv()
    a, b, d = thirds(augmented(xi[...] * scale, True))
    right = jnp.concatenate([a, b, d, a, b, a], axis=0)
    drain_xj.wait_recv()
    a, b, d = thirds(augmented(xj[...] * scale, False))
    left = jnp.concatenate([a, a, a, b, b, d], axis=0)
    step = 2 * block
    for base in range(0, rows * block, step):
        half_distance = lax.dot_general(
            left[:, base:base + step], right, (((0,), (0,)), ((), ())), preferred_element_type=F32
        )
        kt[base:base + step, :] = gain * jnp.exp(jnp.minimum(half_distance, 0.0))

    drain_w = drain(2, vj.at[pl.ds(0, ritz), others_j])
    drain_x0 = drain(4, vj.at[pl.ds(ritz, rhs), others_j])
    drain_wi = drain(3, wi.at[:, others_i])
    drain_w.wait_recv()
    drain_x0.wait_recv()
    ts[...] = dot(vj[...], kt[...])
    ts[pl.ds(0, ritz), lanes(h)] += nugget * w[...]
    ts[pl.ds(ritz, rhs), lanes(h)] += nugget * x0[...] - tgt[...]
    drain_wi.wait_recv()
    gram = dot(wi[...], ts[...], ((1,), (1,)))
    part = ritz // rows
    gram = jnp.concatenate([gram, jnp.zeros((ritz, block - ritz - rhs), F32)], axis=1)
    pscr[...] = gram.reshape(rows, part, block)

    def send_part(k):
        start(6, pscr.at[lax.rem(j + k, rows)], r1.at[me], any_peer(k))

    each(count, send_part)
    each(high, lambda k: start(5, ts.at[:, lanes(lax.rem(h + k, high))], rs1.at[h], col_peer(k)))
    r1[me] = pscr[j]
    rs1[h] = ts[:, lanes(h)]
    drain_r1 = drain(6, r1.at[pl.ds(0, count - 1)])
    drain_r1.wait_recv()
    mine = jnp.sum(r1[...], axis=0)
    sscr[...] = mine
    each(rows, lambda k: start(7, sscr, pfull.at[j], row_peer(k)))
    pfull[j] = mine
    drain_rs1 = drain(5, rs1.at[pl.ds(0, high - 1)])
    drain_rs1.wait_recv()
    own = jnp.sum(rs1[...], axis=0)
    image = own[:ritz]
    drain_pf = drain(7, pfull.at[pl.ds(0, rows - 1)])
    drain_pf.wait_recv()
    full = pfull[...].reshape(ritz, block)

    lane = lax.broadcasted_iota(jnp.int32, (8, block), 1)
    lane_row = lax.broadcasted_iota(jnp.int32, (1, block), 1)
    sub = lax.broadcasted_iota(jnp.int32, (8, block), 0)
    pad = jnp.zeros((block - ritz, block), F32)
    flipped = jnp.concatenate([full, pad], axis=0).T[:ritz]
    tiles = []
    for i in range(ritz // 8):
        top = full[8 * i:8 * i + 8]
        tiles.append(jnp.where(lane < ritz, 0.5 * (top + flipped[8 * i:8 * i + 8]), top))
    wide = 8
    for base in range(0, ritz, wide):
        panel = [[jnp.broadcast_to(t[:, k:k + 1], (8, block)) for t in tiles] for k in range(base, base + wide)]
        for p in range(wide):
            k = base + p
            hold, inner = divmod(k, 8)
            inverse = 1.0 / panel[p][hold][inner:inner + 1]
            pivot_row = jnp.where(lane_row == k, 1.0, tiles[hold][inner:inner + 1]) * inverse
            ahead = [panel[q][hold][inner:inner + 1] * inverse for q in range(p + 1, wide)]
            for i in range(ritz // 8):
                column = panel[p][i]
                kept = jnp.where(lane == k, 0.0, tiles[i])
                later = [panel[q][i] for q in range(p + 1, wide)]
                if i == hold:
                    column = jnp.where(sub == inner, -1.0, column)
                    kept = jnp.where(sub == inner, 0.0, kept)
                    later = [jnp.where(sub == inner, 0.0, value) for value in later]
                tiles[i] = kept - column * pivot_row
                for q, (value, row) in enumerate(zip(later, ahead)):
                    panel[p + 1 + q][i] = value - column * row
    turned = jnp.concatenate(tiles + [pad], axis=0).T
    inverse = turned[:ritz, :ritz]
    amounts = -turned[ritz:ritz + rhs, :ritz]
    moved = dot(amounts, jnp.concatenate([image, w[...]], axis=1))
    residual = -own[ritz:] - moved[:, :block]
    iterate = x0[...] + moved[:, block:]
    against = dot(residual, image, ((1,), (1,)))
    packed = agscr.shape[0]
    agscr[...] = jnp.concatenate([against[i:i + packed] for i in range(0, rhs, packed)], axis=1)
    res[...] = residual
    rj[:, lanes(j)] = residual
    ri[:, lanes(h)] = residual
    each(count, lambda k: start(10, agscr, ag.at[me], any_peer(k)))
    each(rows, lambda k: start(8, res, rj.at[:, lanes(j)], row_peer(k)))
    each(high, lambda k: start(9, res, ri.at[:, lanes(h)], col_peer(k)))
    ag[me] = agscr[...]
    drain_ag = drain(10, ag.at[pl.ds(0, count - 1)])
    drain_rj = drain(8, rj.at[:, others_j])
    drain_ri = drain(9, ri.at[:, others_i])
    drain_ag.wait_recv()
    against = jnp.sum(ag[...], axis=0)
    against = jnp.concatenate([against[:, i:i + ritz] for i in range(0, block, ritz)], axis=0)
    weights = dot(against, inverse)
    drain_rj.wait_recv()
    direction_j = rj[...] - dot(weights, vj[pl.ds(0, ritz), :])
    drain_ri.wait_recv()
    direction_i = ri[...] - dot(weights, wi[...])
    dscr[...] = direction_i
    direction = dscr[:, lanes(h)]
    applied_i = dot(direction_j, kt[...])
    ts2[...] = applied_i
    ts2[:, lanes(h)] += nugget * direction
    each(high, lambda k: start(11, ts2.at[:, lanes(lax.rem(h + k, high))], rs2.at[h], col_peer(k)))
    curve = jnp.sum(ts2[...] * direction_i, axis=1, keepdims=True)
    squares = jnp.sum(residual * residual, axis=1, keepdims=True)
    lane = lax.broadcasted_iota(jnp.int32, (rhs, block), 1)
    sub = lax.broadcasted_iota(jnp.int32, (rhs, block), 0)
    cscr[...] = jnp.sum(
        jnp.where(lane == sub, curve, jnp.where(lane == sub + rhs, squares, 0.0)), axis=0, keepdims=True
    )
    each(count, lambda k: start(12, cscr, cv.at[me], any_peer(k)))
    cv[me] = cscr[...]
    rs2[h] = ts2[:, lanes(h)]
    drain_rs2 = drain(11, rs2.at[pl.ds(0, high - 1)])
    drain_cv = drain(12, cv.at[pl.ds(0, count - 1)])
    drain_rs2.wait_recv()
    applied = jnp.sum(rs2[...], axis=0)
    drain_cv.wait_recv()
    totals = jnp.broadcast_to(jnp.sum(cv[...], axis=0), (rhs, block))
    curve = jnp.sum(jnp.where(lane == sub, totals, 0.0), axis=1, keepdims=True)
    squares = jnp.sum(jnp.where(lane == sub + rhs, totals, 0.0), axis=1, keepdims=True)
    step_size = squares / curve
    out[pl.ds(0, rhs)] = iterate + step_size * direction
    out[pl.ds(rhs, rhs)] = residual - step_size * applied
    for item in (drain_rj, drain_ri, drain_xj, drain_xi, drain_w, drain_wi, drain_x0, drain_rs1, drain_r1, drain_pf,
                 drain_ag, drain_rs2, drain_cv):
        item.wait_send()


def local(high, low, cols, points, inv_scales, amplitude, noise_var, targets, initial, ritz_basis):
    feat, block = points.shape
    rhs = initial.shape[0]
    ritz = ritz_basis.shape[0]
    rows = low * cols
    count = high * rows
    vectors = rhs + ritz
    part = ritz // rows
    packed = rhs * ritz // block
    scratch = [
        VMEM((feat, block), F32),
        SMEM((feat,), F32),
        SMEM((1,), F32),
        SMEM((1,), F32),
        VMEM((rhs, block), F32),
        VMEM((rhs, block), F32),
        VMEM((ritz, block), F32),
        VMEM((rhs, block), F32),
        VMEM((feat, rows * block), F32),
        VMEM((feat, high * block), F32),
        VMEM((vectors, rows * block), F32),
        VMEM((ritz, high * block), F32),
        VMEM((rows * block, high * block), F32),
        VMEM((vectors, high * block), F32),
        VMEM((high, vectors, block), F32),
        VMEM((rows, part, block), F32),
        VMEM((count, part, block), F32),
        VMEM((rows, part, block), F32),
        VMEM((part, block), F32),
        VMEM((rhs, rows * block), F32),
        VMEM((rhs, high * block), F32),
        VMEM((packed, block), F32),
        VMEM((count, packed, block), F32),
        VMEM((rhs, high * block), F32),
        VMEM((rhs, high * block), F32),
        VMEM((high, rhs, block), F32),
        VMEM((1, block), F32),
        VMEM((count, 1, block), F32),
        pltpu.SemaphoreType.DMA((7,)),
        pltpu.SemaphoreType.DMA((13,)),
        pltpu.SemaphoreType.DMA((13,)),
    ]
    hbm = pl.BlockSpec(memory_space=pltpu.HBM)
    out = pl.pallas_call(
        functools.partial(kernel, high, low, cols),
        out_shape=jax.ShapeDtypeStruct((2 * rhs, block), F32),
        in_specs=[hbm] * 7,
        out_specs=pl.BlockSpec(memory_space=VMEM),
        scratch_shapes=scratch,
        compiler_params=pltpu.CompilerParams(
            collective_id=0, has_side_effects=True
        ),
        name="deflated_cg",
    )(points, inv_scales, amplitude, noise_var, targets, initial, ritz_basis)
    return out[:rhs], out[rhs:]


def solution(mesh):
    spread = P(None, ("col", "row"))
    rows, cols = mesh.shape["row"], mesh.shape["col"]
    low = next(d for d in range(1, rows + 1) if rows % d == 0 and d * cols >= rows // d)
    return jax.shard_map(
        functools.partial(local, rows // low, low, cols),
        mesh=mesh,
        in_specs=(spread, P(), P(), P(), spread, spread, spread),
        out_specs=(spread, spread),
        check_vma=False,
    )
```
